32 devices in a mesh: dp: 4 (over z), head: 8 (over y, x, core).
Axes of the slice: x: 2, y: 2, z: 4, core: 2. Of those that a mesh axis runs over, the one named last changes fastest.
Arguments:
- projected: bfloat16 [12288, 24576], P(('dp', 'head')), may hold values from -64 to 64, as said below
- weight_exp: int32 [12288], P(('dp', 'head')), may hold values from 0 to 3
- damp_exp: int32 [128], replicated, may hold values from 0 to 2
Outputs:
- whitening: float32 [128, 192, 192], P('head')
The draws below stay inside these ranges and needn't reach their ends.
Inputs may be any that keep to these rules, and one draw needn't show every extreme that they name: `projected`: real values.
All inputs are finite; a program needn't handle non-finite values.
Results may differ from the reference program's by a relative error of at most 0.0003.
Values may be sent and summed in bfloat16 or wider, within the bound.
A program may use at most 192 MiB of HBM per device.

```python
import math
import jax
import jax.numpy as jnp
from jax import lax

HEADS = 64
HD = 192
TOKENS = 12288
MATS = 128


def draw_projected(key, part):
    first, second = jax.random.split(jax.random.fold_in(key, 11))
    base = jax.random.normal(first, (TOKENS, 2 * HEADS, HD), jnp.float32)
    scales = jnp.exp(jax.random.uniform(second, (2 * HEADS, HD), jnp.float32, 0.0, math.log(8.0)))
    mixed = base + 0.6 * jnp.roll(base, 1, axis=2) - 0.4 * jnp.roll(base, 5, axis=2)
    return jnp.clip((mixed * scales).reshape(TOKENS, 2 * HEADS * HD) / 4.0, -64.0, 64.0).astype(jnp.bfloat16)


def place_ends(entries, own_key, smallest, largest):
    longest = entries.shape.index(max(entries.shape))
    spots = []
    for shift in (0, 1):
        where = [jax.random.randint(jax.random.fold_in(own_key, axis), (), 0, length) for axis, length in enumerate(entries.shape)]
        where[longest] = (where[longest] + shift) % entries.shape[longest]
        spots.append(tuple(where))
    return entries.at[spots[0]].set(smallest).at[spots[1]].set(largest)


def setup_inputs(seed: int = 0) -> dict:
    seeds = jax.random.split(jax.random.key(seed), 4)
    return {
        "projected": draw_projected(jax.random.fold_in(seeds[3], 71), 0),
        "weight_exp": place_ends(jax.random.randint(seeds[1], (TOKENS,), 0, 4), jax.random.fold_in(seeds[1], 1), 0, 3).astype(jnp.int32),
        "damp_exp": place_ends(jax.random.randint(seeds[2], (MATS,), 0, 3), jax.random.fold_in(seeds[2], 1), 0, 2).astype(jnp.int32),
    }


def reference(projected, weight_exp, damp_exp):
    mats = projected.shape[1] // HD
    weights = jnp.exp2(weight_exp.astype(jnp.float32)).astype(jnp.bfloat16)
    scaled = projected * weights[:, None]
    eye = jnp.eye(HD, dtype=jnp.float32)

    def single(index):
        start = (index * HD).astype(jnp.int32)
        left = lax.dynamic_slice_in_dim(projected, start, HD, 1)
        right = lax.dynamic_slice_in_dim(scaled, start, HD, 1)
        gram = jnp.dot(left.T.astype(jnp.float32), right.astype(jnp.float32), preferred_element_type=jnp.float32) / TOKENS
        gram = 0.5 * (gram + gram.T)
        level = jnp.trace(gram) / HD + 1e-06
        damping = jnp.exp2(-damp_exp[index].astype(jnp.float32)) * level
        lower = jnp.linalg.cholesky(gram + damping * eye)
        return jax.scipy.linalg.solve_triangular(lower, eye, lower=True)
    return lax.map(single, jnp.arange(mats, dtype=jnp.int32))
```

```python
import functools

import jax
import jax.numpy as jnp
from jax import lax
from jax.experimental import pallas as pl
from jax.experimental.pallas import tpu as pltpu
from jax.sharding import PartitionSpec as P

HD = 192
BLK = HD // 3
HIGH = lax.Precision.HIGHEST


def gram_kernel(rows_ref, weights_ref, out_ref):
    rows = rows_ref[...]
    weighted = rows * weights_ref[...]
    contract = (((0,), (0,)), ((), ()))
    width = 4 * BLK
    first = lax.dot_general(rows[:, :width], weighted[:, :width], contract, preferred_element_type=jnp.float32)
    second = lax.dot_general(rows[:, -width:], weighted[:, -width:], contract, preferred_element_type=jnp.float32)
    two = 2 * BLK
    lanes = lax.broadcasted_iota(jnp.int32, (BLK, two), 1)
    corner = pltpu.roll(first[two : two + BLK, two:], BLK, 1)
    out_ref[0, :BLK, :] = jnp.where(lanes < BLK, first[:BLK, :two], corner)
    out_ref[0, BLK:, :] = first[BLK:HD, :two]
    out_ref[1, :two, :] = second[BLK : BLK + two, two:]
    corner = pltpu.roll(second[BLK:two, :two], BLK, 1)
    out_ref[1, two:, :] = jnp.where(lanes < BLK, corner, second[HD:, two:])


def packed_grams(projected, weights):
    tokens, columns = projected.shape
    mats = columns // HD
    return pl.pallas_call(
        gram_kernel,
        grid=(mats // 2,),
        in_specs=[
            pl.BlockSpec((tokens, 2 * HD), lambda i: (0, i)),
            pl.BlockSpec((tokens, 1), lambda i: (0, 0)),
        ],
        out_specs=pl.BlockSpec((2, HD, 2 * BLK), lambda i: (i, 0, 0)),
        out_shape=jax.ShapeDtypeStruct((mats, HD, 2 * BLK), jnp.float32),
    )(projected, weights)


def dot(a, b):
    return lax.dot_general(a, b, (((1,), (0,)), ((), ())), precision=HIGH, preferred_element_type=jnp.float32)


def dot_t(a, b):
    return lax.dot_general(a, b, (((1,), (1,)), ((), ())), precision=HIGH, preferred_element_type=jnp.float32)


def inverse_factors(blocks):
    lane = lax.broadcasted_iota(jnp.int32, (8, BLK), 1)
    sub = lax.broadcasted_iota(jnp.int32, (8, BLK), 0)
    sub1 = lax.broadcasted_iota(jnp.int32, (8, 1), 0)
    groups = BLK // 8
    held = [[block[8 * g : 8 * g + 8] for g in range(groups)] for block in blocks]
    for k in range(BLK):
        own, spot = divmod(k, 8)
        is_k = lane == k
        for parts in held:
            row = parts[own][spot : spot + 1, :]
            scale = 1.0 / row[:, k : k + 1]
            row = jnp.where(is_k[:1], 1.0, row) * scale
            for g in range(own, groups):
                part = parts[g]
                column = part[:, k : k + 1]
                if g == own:
                    if spot == 7:
                        continue
                    column = jnp.where(sub1 > spot, column, 0.0)
                    kept = jnp.where(is_k & (sub > spot), 0.0, part)
                else:
                    kept = jnp.where(is_k, 0.0, part)
                parts[g] = kept - column * row
    out = []
    for parts in held:
        rows = []
        for g in range(groups):
            ids = sub + 8 * g
            pivot = jnp.sum(jnp.where(lane == ids, parts[g], 0.0), axis=1, keepdims=True)
            unit = jnp.where(lane < ids, parts[g], jnp.where(lane == ids, 1.0, 0.0))
            rows.append(unit * (1.0 / jnp.sqrt(pivot)))
        out.append(jnp.concatenate(rows, axis=0))
    return out


def whiten_kernel(total, count, damp_ref, packed_ref, out_ref):
    two = 2 * BLK
    diag = lax.broadcasted_iota(jnp.int32, (BLK, BLK), 0) == lax.broadcasted_iota(jnp.int32, (BLK, BLK), 1)
    a11, a22, a33, low, a32 = [], [], [], [], []
    for m in range(count):
        got = packed_ref[m] / total
        if m % 2 == 0:
            d1, d3 = got[:BLK, :BLK], got[:BLK, BLK:]
            d2 = got[BLK:two, BLK:]
            left = got[BLK:, :BLK]
            corner = got[two:, BLK:]
        else:
            left = got[:BLK, :].T
            d2 = got[BLK:two, :BLK]
            corner = got[BLK:two, BLK:].T
            d1, d3 = got[two:, :BLK], got[two:, BLK:]
        trace = jnp.sum(jnp.where(diag, d1 + d2 + d3, 0.0), axis=(0, 1), keepdims=True)
        level = trace / HD + 1e-06
        shift = jnp.where(diag, damp_ref[m] * level, 0.0)
        a11.append(d1 + shift)
        a22.append(d2 + shift)
        a33.append(d3 + shift)
        low.append(left)
        a32.append(corner)
    each = range(count)
    w11 = inverse_factors(a11)
    l1 = [dot_t(low[m], w11[m]) for m in each]
    square = [dot_t(l1[m], l1[m]) for m in each]
    w22 = inverse_factors([a22[m] - square[m][:BLK, :BLK] for m in each])
    l32 = [dot_t(a32[m] - square[m][BLK:, :BLK], w22[m]) for m in each]
    w33 = inverse_factors([a33[m] - square[m][BLK:, BLK:] - dot_t(l32[m], l32[m]) for m in each])
    zero = jnp.zeros((BLK, BLK), jnp.float32)
    for m in each:
        below = dot(l1[m], w11[m])
        w21 = -dot(w22[m], below[:BLK])
        w32 = -dot(w33[m], dot(l32[m], w22[m]))
        w31 = -dot(w33[m], below[BLK:] + dot(l32[m], w21))
        out_ref[m, :BLK, :two] = jnp.concatenate((w11[m], zero), axis=1)
        out_ref[m, BLK:two, :two] = jnp.concatenate((w21, w22[m]), axis=1)
        out_ref[m, two:, :two] = jnp.concatenate((w31, w32), axis=1)
        out_ref[m, :two, two:] = jnp.zeros((two, BLK), jnp.float32)
        out_ref[m, two:, two:] = w33[m]


def whiten(packed, damp, total):
    count = packed.shape[0]
    return pl.pallas_call(
        functools.partial(whiten_kernel, total, count),
        in_specs=[pl.BlockSpec(memory_space=pltpu.SMEM), pl.BlockSpec(memory_space=pltpu.VMEM)],
        out_specs=pl.BlockSpec(memory_space=pltpu.VMEM),
        out_shape=jax.ShapeDtypeStruct((count, HD, HD), jnp.float32),
    )(damp, packed)


def on_device(projected, weight_exp, damp_exp):
    n_head = lax.axis_size("head")
    n_dp = lax.axis_size("dp")
    mats = projected.shape[1] // HD
    share = mats // (n_head * n_dp)
    total = projected.shape[0] * n_head * n_dp
    weights = jnp.exp2(weight_exp.astype(jnp.float32)).astype(jnp.bfloat16)
    packed = packed_grams(projected, weights[:, None])
    part = lax.psum_scatter(packed, "head", scatter_dimension=0, tiled=True)
    owned = lax.psum_scatter(part, "dp", scatter_dimension=0, tiled=True)
    first = (lax.axis_index("head") * n_dp + lax.axis_index("dp")) * share
    damp = jnp.exp2(-lax.dynamic_slice_in_dim(damp_exp, first, share, 0).astype(jnp.float32))
    factors = whiten(owned, damp, float(total))
    return lax.all_gather(factors, "dp", axis=0, tiled=True)


def solution(mesh):
    return jax.shard_map(
        on_device,
        mesh=mesh,
        in_specs=(P(("dp", "head"), None), P(("dp", "head")), P()),
        out_specs=P("head", None, None),
        check_vma=False,
    )
```

```python
import functools

import jax
import jax.numpy as jnp
from jax import lax
from jax.experimental import pallas as pl
from jax.experimental.pallas import tpu as pltpu
from jax.sharding import PartitionSpec as P

HD = 192
BLK = HD // 3
HIGH = lax.Precision.HIGHEST


def gram_kernel(rows_ref, weights_ref, out_ref):
    rows = rows_ref[...]
    weighted = rows * weights_ref[...]
    contract = (((0,), (0,)), ((), ()))
    width = 4 * BLK
    first = lax.dot_general(rows[:, :width], weighted[:, :width], contract, preferred_element_type=jnp.float32)
    second = lax.dot_general(rows[:, -width:], weighted[:, -width:], contract, preferred_element_type=jnp.float32)
    two = 2 * BLK
    lanes = lax.broadcasted_iota(jnp.int32, (BLK, two), 1)
    corner = pltpu.roll(first[two : two + BLK, two:], BLK, 1)
    out_ref[0, :BLK, :] = jnp.where(lanes < BLK, first[:BLK, :two], corner)
    out_ref[0, BLK:, :] = first[BLK:HD, :two]
    out_ref[1, :two, :] = second[BLK : BLK + two, two:]
    corner = pltpu.roll(second[BLK:two, :two], BLK, 1)
    out_ref[1, two:, :] = jnp.where(lanes < BLK, corner, second[HD:, two:])


def packed_grams(projected, weights):
    tokens, columns = projected.shape
    mats = columns // HD
    return pl.pallas_call(
        gram_kernel,
        grid=(mats // 2,),
        in_specs=[
            pl.BlockSpec((tokens, 2 * HD), lambda i: (0, i)),
            pl.BlockSpec((tokens, 1), lambda i: (0, 0)),
        ],
        out_specs=pl.BlockSpec((2, HD, 2 * BLK), lambda i: (i, 0, 0)),
        out_shape=jax.ShapeDtypeStruct((mats, HD, 2 * BLK), jnp.float32),
    )(projected, weights)


def dot(a, b):
    return lax.dot_general(a, b, (((1,), (0,)), ((), ())), precision=HIGH, preferred_element_type=jnp.float32)


def dot_t(a, b):
    return lax.dot_general(a, b, (((1,), (1,)), ((), ())), precision=HIGH, preferred_element_type=jnp.float32)


def inverse_factors(blocks):
    lane = lax.broadcasted_iota(jnp.int32, (8, BLK), 1)
    sub = lax.broadcasted_iota(jnp.int32, (8, BLK), 0)
    sub1 = lax.broadcasted_iota(jnp.int32, (8, 1), 0)
    groups = BLK // 8
    held = [[block[8 * g : 8 * g + 8] for g in range(groups)] for block in blocks]
    for k in range(BLK):
        own, spot = divmod(k, 8)
        is_k = lane == k
        for parts in held:
            row = parts[own][spot : spot + 1, :]
            scale = 1.0 / row[:, k : k + 1]
            row = jnp.where(is_k[:1], 1.0, row) * scale
            for g in range(own, groups):
                part = parts[g]
                column = part[:, k : k + 1]
                if g == own:
                    if spot == 7:
                        continue
                    column = jnp.where(sub1 > spot, column, 0.0)
                    kept = jnp.where(is_k & (sub > spot), 0.0, part)
                else:
                    kept = jnp.where(is_k, 0.0, part)
                parts[g] = kept - column * row
    out = []
    for parts in held:
        rows = []
        for g in range(groups):
            ids = sub + 8 * g
            pivot = jnp.sum(jnp.where(lane == ids, parts[g], 0.0), axis=1, keepdims=True)
            unit = jnp.where(lane < ids, parts[g], jnp.where(lane == ids, 1.0, 0.0))
            rows.append(unit * (1.0 / jnp.sqrt(pivot)))
        out.append(jnp.concatenate(rows, axis=0))
    return out


def unpack_even(got):
    two = 2 * BLK
    return got[:BLK, :BLK], got[BLK:two, BLK:], got[:BLK, BLK:], got[BLK:, :BLK], got[two:, BLK:]


def unpack_odd(got):
    two = 2 * BLK
    return got[two:, :BLK], got[BLK:two, :BLK], got[two:, BLK:], got[:BLK, :].T, got[BLK:two, BLK:].T


def whiten_kernel(total, count, damp_ref, packed_ref, out_ref):
    two = 2 * BLK
    diag = lax.broadcasted_iota(jnp.int32, (BLK, BLK), 0) == lax.broadcasted_iota(jnp.int32, (BLK, BLK), 1)
    a11, a22, a33, low, a32 = [], [], [], [], []
    for m in range(count):
        got = packed_ref[m] / total
        even = unpack_even(got)
        odd = unpack_odd(got)
        if count % 2 == 0:
            d1, d2, d3, left, corner = odd if m % 2 else even
        else:
            turn = (lax.axis_index("head") * lax.axis_size("dp") + lax.axis_index("dp")) * count + m
            d1, d2, d3, left, corner = (jnp.where(turn % 2 == 0, a, b) for a, b in zip(even, odd))
        trace = jnp.sum(jnp.where(diag, d1 + d2 + d3, 0.0), axis=(0, 1), keepdims=True)
        level = trace / HD + 1e-06
        shift = jnp.where(diag, damp_ref[m] * level, 0.0)
        a11.append(d1 + shift)
        a22.append(d2 + shift)
        a33.append(d3 + shift)
        low.append(left)
        a32.append(corner)
    each = range(count)
    w11 = inverse_factors(a11)
    l1 = [dot_t(low[m], w11[m]) for m in each]
    square = [dot_t(l1[m], l1[m]) for m in each]
    w22 = inverse_factors([a22[m] - square[m][:BLK, :BLK] for m in each])
    l32 = [dot_t(a32[m] - square[m][BLK:, :BLK], w22[m]) for m in each]
    w33 = inverse_factors([a33[m] - square[m][BLK:, BLK:] - dot_t(l32[m], l32[m]) for m in each])
    for m in each:
        below = dot(l1[m], w11[m])
        w21 = -dot(w22[m], below[:BLK])
        w32 = -dot(w33[m], dot(l32[m], w22[m]))
        w31 = -dot(w33[m], below[BLK:] + dot(l32[m], w21))
        out_ref[m, :BLK] = jnp.concatenate((w11[m], w33[m]), axis=1)
        out_ref[m, BLK:two] = jnp.concatenate((w21, w22[m]), axis=1)
        out_ref[m, two:] = jnp.concatenate((w31, w32), axis=1)


def whiten(packed, damp, total):
    count = packed.shape[0]
    return pl.pallas_call(
        functools.partial(whiten_kernel, total, count),
        in_specs=[pl.BlockSpec(memory_space=pltpu.SMEM), pl.BlockSpec(memory_space=pltpu.VMEM)],
        out_specs=pl.BlockSpec(memory_space=pltpu.VMEM),
        out_shape=jax.ShapeDtypeStruct(packed.shape, jnp.float32),
    )(damp, packed)


def flip(index, step):
    return index + step * (1 - 2 * ((index // step) % 2))


def remote(src, dst, sems, slot, device):
    return pltpu.make_async_remote_copy(
        src_ref=src,
        dst_ref=dst,
        send_sem=sems.at[0, slot],
        recv_sem=sems.at[1, slot],
        device_id=device,
        device_id_type=pl.DeviceIdType.MESH,
    )


def greet(heads, dps):
    barrier = pltpu.get_barrier_semaphore()
    for peer in heads:
        pl.semaphore_signal(barrier, inc=1, device_id={"head": peer}, device_id_type=pl.DeviceIdType.MESH)
    for peer in dps:
        pl.semaphore_signal(barrier, inc=1, device_id={"dp": peer}, device_id_type=pl.DeviceIdType.MESH)
    pl.semaphore_wait(barrier, len(heads) + len(dps))


def part_rows():
    last = HD // 4
    first = (HD - last) // 2
    return (0, first), (first, first), (2 * first, last)


def scatter_kernel(n_head, n_dp, share, packed_ref, out_ref, acc, got_a, got_b, got_c, got_z, got_y, sem_0, sem_a, sem_b, sem_c, sem_z, sem_y):
    head = lax.axis_index("head")
    dp = lax.axis_index("dp")
    chunks = n_head // 2
    bits = chunks.bit_length() - 1
    mine = head // 2
    core = head % 2
    per_head = share * n_dp
    peers = [lax.rem(dp + o, n_dp) for o in range(1, n_dp)]
    greet([flip(head, 1 << j) for j in range(bits + 1)], peers)

    pair = []
    for c in range(chunks):
        theirs = (2 * c + 1 - core) * per_head
        copy = remote(packed_ref.at[pl.ds(theirs, per_head)], acc.at[c], sem_0, c, {"head": flip(head, 1)})
        copy.start()
        pair.append(copy)
    for c in range(chunks):
        pair[c].wait()
        base = (2 * c + core) * per_head

        def add(m, carry, c=c, base=base):
            acc[c, m] += packed_ref[base + m]
            return carry

        lax.fori_loop(0, per_head, add, 0)

    def begin(part, got, sems, order, step, first, count):
        j = order[step]
        bit = (mine // (1 << j)) % 2
        fixed = 0
        for done in order[:step]:
            fixed = fixed + (mine // (1 << done)) % 2 * (1 << done)
        free = [b for b in range(bits) if b not in order[: step + 1]]
        flight = []
        start, size = part
        offset = sum(chunks >> (s + 1) for s in range(step))
        for e in range(1 << len(free)):
            base = fixed + sum(((e >> i) & 1) << b for i, b in enumerate(free))
            slot = offset + e
            copy = remote(
                acc.at[base + (1 - bit) * (1 << j), pl.ds(first, count), pl.ds(start, size)],
                got.at[slot],
                sems,
                slot,
                {"head": flip(head, 2 << j)},
            )
            copy.start()
            flight.append((copy, base + bit * (1 << j), slot))
        return flight, part, got, first, count

    def finish(state):
        flight, (start, size), got, first, count = state
        for copy, keep, slot in flight:
            copy.wait()

            def add(m, carry, keep=keep, slot=slot):
                acc[keep, first + m, start : start + size] += got[slot, m]
                return carry

            lax.fori_loop(0, count, add, 0)

    part_a, part_b, part_c = part_rows()
    up = list(range(bits))
    down = up[::-1]
    rows_c = pl.ds(part_c[0], part_c[1])
    own = dp * share
    flight_z = []
    for step in range(bits):
        state_a = begin(part_a, got_a, sem_a, up, step, 0, per_head)
        state_b = begin(part_b, got_b, sem_b, down, step, 0, per_head)
        if step == 0:
            for o, peer in enumerate(peers):
                copy = remote(acc.at[:, pl.ds(peer * share, share), rows_c], got_z.at[o], sem_z, o, {"dp": peer})
                copy.start()
                flight_z.append(copy)
        finish(state_a)
        finish(state_b)
    rows_ab = pl.ds(0, part_c[0])
    flight_y = []
    for o, peer in enumerate(peers):
        copy = remote(acc.at[mine, pl.ds(peer * share, share), rows_ab], got_y.at[o], sem_y, o, {"dp": peer})
        copy.start()
        flight_y.append(copy)
    for copy in flight_z:
        copy.wait()
    for c in range(chunks):

        def add_z(m, carry, c=c):
            value = acc[c, own + m, part_c[0] :]
            for o in range(len(peers)):
                value += got_z[o, c, m]
            acc[c, own + m, part_c[0] :] = value
            return carry

        lax.fori_loop(0, share, add_z, 0)
    for step in range(bits):
        finish(begin(part_c, got_c, sem_c, up, step, own, share))
    for copy in flight_y:
        copy.wait()

    def add_y(m, carry):
        value = acc[mine, own + m, : part_c[0]]
        for o in range(len(peers)):
            value += got_y[o, m]
        out_ref[m, : part_c[0]] = value
        out_ref[m, part_c[0] :] = acc[mine, own + m, part_c[0] :]
        return carry

    lax.fori_loop(0, share, add_y, 0)


def scatter_sum(packed, n_head, n_dp):
    mats, rows, lanes = packed.shape
    per_head = mats // n_head
    share = per_head // n_dp
    chunks = n_head // 2
    (_, rows_a), (_, rows_b), (_, rows_c) = part_rows()
    f32 = jnp.float32
    return pl.pallas_call(
        functools.partial(scatter_kernel, n_head, n_dp, share),
        in_specs=[pl.BlockSpec(memory_space=pltpu.VMEM)],
        out_specs=pl.BlockSpec(memory_space=pltpu.VMEM),
        out_shape=jax.ShapeDtypeStruct((share, rows, lanes), f32),
        scratch_shapes=[
            pltpu.VMEM((chunks, per_head, rows, lanes), f32),
            pltpu.VMEM((chunks - 1, per_head, rows_a, lanes), f32),
            pltpu.VMEM((chunks - 1, per_head, rows_b, lanes), f32),
            pltpu.VMEM((chunks - 1, share, rows_c, lanes), f32),
            pltpu.VMEM((n_dp - 1, chunks, share, rows_c, lanes), f32),
            pltpu.VMEM((n_dp - 1, share, rows - rows_c, lanes), f32),
            pltpu.SemaphoreType.DMA((2, chunks)),
            pltpu.SemaphoreType.DMA((2, chunks - 1)),
            pltpu.SemaphoreType.DMA((2, chunks - 1)),
            pltpu.SemaphoreType.DMA((2, chunks - 1)),
            pltpu.SemaphoreType.DMA((2, n_dp - 1)),
            pltpu.SemaphoreType.DMA((2, n_dp - 1)),
        ],
        compiler_params=pltpu.CompilerParams(collective_id=0, has_side_effects=True, vmem_limit_bytes=60 << 20),
    )(packed)


def gather_kernel(n_dp, share, packed_ref, out_ref, got, sems):
    dp = lax.axis_index("dp")
    peers = [lax.rem(dp + o, n_dp) for o in range(1, n_dp)]
    greet([], peers)
    flight = []
    for o, peer in enumerate(peers):
        copy = remote(packed_ref, got.at[o], sems, o, {"dp": peer})
        copy.start()
        flight.append(copy)
    two = 2 * BLK

    def unpack(source, base):
        def one(m, carry):
            top = source[m, :BLK]
            out_ref[base + m, :BLK, :two] = jnp.where(lax.broadcasted_iota(jnp.int32, (BLK, two), 1) < BLK, top, 0.0)
            out_ref[base + m, BLK:, :two] = source[m, BLK:]
            out_ref[base + m, :two, two:] = jnp.zeros((two, BLK), jnp.float32)
            out_ref[base + m, two:, two:] = top[:, BLK:]
            return carry

        lax.fori_loop(0, share, one, 0)

    unpack(packed_ref, dp * share)
    for o in range(n_dp - 1):
        flight[o].wait()
        unpack(got.at[o], lax.rem(dp + n_dp - 1 - o, n_dp) * share)


def gather(packed, n_dp):
    share, rows, lanes = packed.shape
    return pl.pallas_call(
        functools.partial(gather_kernel, n_dp, share),
        in_specs=[pl.BlockSpec(memory_space=pltpu.VMEM)],
        out_specs=pl.BlockSpec(memory_space=pltpu.VMEM),
        out_shape=jax.ShapeDtypeStruct((n_dp * share, HD, HD), jnp.float32),
        scratch_shapes=[
            pltpu.VMEM((n_dp - 1, share, rows, lanes), jnp.float32),
            pltpu.SemaphoreType.DMA((2, n_dp - 1)),
        ],
        compiler_params=pltpu.CompilerParams(collective_id=1, has_side_effects=True),
    )(packed)


def on_device(projected, weight_exp, damp_exp):
    n_head = lax.axis_size("head")
    n_dp = lax.axis_size("dp")
    mats = projected.shape[1] // HD
    share = mats // (n_head * n_dp)
    total = projected.shape[0] * n_head * n_dp
    weights = jnp.exp2(weight_exp.astype(jnp.float32)).astype(jnp.bfloat16)
    packed = packed_grams(projected, weights[:, None])
    owned = scatter_sum(packed, n_head, n_dp)
    first = (lax.axis_index("head") * n_dp + lax.axis_index("dp")) * share
    damp = jnp.exp2(-lax.dynamic_slice_in_dim(damp_exp, first, share, 0).astype(jnp.float32))
    factors = whiten(owned, damp, float(total))
    return gather(factors, n_dp)


def solution(mesh):
    return jax.shard_map(
        on_device,
        mesh=mesh,
        in_specs=(P(("dp", "head"), None), P(("dp", "head")), P()),
        out_specs=P("head", None, None),
        check_vma=False,
    )
```

```python
import functools

import jax
import jax.numpy as jnp
from jax import lax
from jax.experimental import pallas as pl
from jax.experimental.pallas import tpu as pltpu
from jax.sharding import PartitionSpec as P

HD = 192
BLK = HD // 3
HIGH = lax.Precision.HIGHEST


def store_pair(rows, wide, out, at):
    weighted = rows * wide
    contract = (((0,), (0,)), ((), ()))
    width = 4 * BLK
    first = lax.dot_general(rows[:, :width], weighted[:, :width], contract, preferred_element_type=jnp.float32)
    second = lax.dot_general(rows[:, -width:], weighted[:, -width:], contract, preferred_element_type=jnp.float32)
    two = 2 * BLK
    lanes = lax.broadcasted_iota(jnp.int32, (BLK, two), 1)
    corner = pltpu.roll(first[two : two + BLK, two:], BLK, 1)
    out[at, :BLK, :] = jnp.where(lanes < BLK, first[:BLK, :two], corner)
    out[at, BLK:, :] = first[BLK:HD, :two]
    out[at + 1, :two, :] = second[BLK : BLK + two, two:]
    corner = pltpu.roll(second[BLK:two, :two], BLK, 1)
    out[at + 1, two:, :] = jnp.where(lanes < BLK, corner, second[HD:, two:])


def dot(a, b):
    return lax.dot_general(a, b, (((1,), (0,)), ((), ())), precision=HIGH, preferred_element_type=jnp.float32)


def dot_t(a, b):
    return lax.dot_general(a, b, (((1,), (1,)), ((), ())), precision=HIGH, preferred_element_type=jnp.float32)


def inverse_factors(blocks):
    lane = lax.broadcasted_iota(jnp.int32, (8, BLK), 1)
    sub = lax.broadcasted_iota(jnp.int32, (8, BLK), 0)
    sub1 = lax.broadcasted_iota(jnp.int32, (8, 1), 0)
    groups = BLK // 8
    held = [[block[8 * g : 8 * g + 8] for g in range(groups)] for block in blocks]
    for k in range(BLK):
        own, spot = divmod(k, 8)
        is_k = lane == k
        for parts in held:
            row = parts[own][spot : spot + 1, :]
            scale = 1.0 / row[:, k : k + 1]
            row = jnp.where(is_k[:1], 1.0, row) * scale
            for g in range(own, groups):
                part = parts[g]
                column = part[:, k : k + 1]
                if g == own:
                    if spot == 7:
                        continue
                    column = jnp.where(sub1 > spot, column, 0.0)
                    kept = jnp.where(is_k & (sub > spot), 0.0, part)
                else:
                    kept = jnp.where(is_k, 0.0, part)
                parts[g] = kept - column * row
    out = []
    for parts in held:
        rows = []
        for g in range(groups):
            ids = sub + 8 * g
            pivot = jnp.sum(jnp.where(lane == ids, parts[g], 0.0), axis=1, keepdims=True)
            unit = jnp.where(lane < ids, parts[g], jnp.where(lane == ids, 1.0, 0.0))
            rows.append(unit * (1.0 / jnp.sqrt(pivot)))
        out.append(jnp.concatenate(rows, axis=0))
    return out


def unpack_even(got):
    two = 2 * BLK
    return got[:BLK, :BLK], got[BLK:two, BLK:], got[:BLK, BLK:], got[BLK:, :BLK], got[two:, BLK:]


def unpack_odd(got):
    two = 2 * BLK
    return got[two:, :BLK], got[BLK:two, :BLK], got[two:, BLK:], got[:BLK, :].T, got[BLK:two, BLK:].T


def whiten_kernel(total, count, damp_ref, packed_ref, out_ref):
    two = 2 * BLK
    diag = lax.broadcasted_iota(jnp.int32, (BLK, BLK), 0) == lax.broadcasted_iota(jnp.int32, (BLK, BLK), 1)
    a11, a22, a33, low, a32 = [], [], [], [], []
    for m in range(count):
        got = packed_ref[m] / total
        even = unpack_even(got)
        odd = unpack_odd(got)
        if count % 2 == 0:
            d1, d2, d3, left, corner = odd if m % 2 else even
        else:
            turn = (lax.axis_index("head") * lax.axis_size("dp") + lax.axis_index("dp")) * count + m
            d1, d2, d3, left, corner = (jnp.where(turn % 2 == 0, a, b) for a, b in zip(even, odd))
        trace = jnp.sum(jnp.where(diag, d1 + d2 + d3, 0.0), axis=(0, 1), keepdims=True)
        level = trace / HD + 1e-06
        shift = jnp.where(diag, damp_ref[m] * level, 0.0)
        a11.append(d1 + shift)
        a22.append(d2 + shift)
        a33.append(d3 + shift)
        low.append(left)
        a32.append(corner)
    each = range(count)
    w11 = inverse_factors(a11)
    l1 = [dot_t(low[m], w11[m]) for m in each]
    square = [dot_t(l1[m], l1[m]) for m in each]
    w22 = inverse_factors([a22[m] - square[m][:BLK, :BLK] for m in each])
    l32 = [dot_t(a32[m] - square[m][BLK:, :BLK], w22[m]) for m in each]
    w33 = inverse_factors([a33[m] - square[m][BLK:, BLK:] - dot_t(l32[m], l32[m]) for m in each])
    for m in each:
        below = dot(l1[m], w11[m])
        w21 = -dot(w22[m], below[:BLK])
        w32 = -dot(w33[m], dot(l32[m], w22[m]))
        w31 = -dot(w33[m], below[BLK:] + dot(l32[m], w21))
        out_ref[m, :BLK] = jnp.concatenate((w11[m], w33[m]), axis=1)
        out_ref[m, BLK:two] = jnp.concatenate((w21, w22[m]), axis=1)
        out_ref[m, two:] = jnp.concatenate((w31, w32), axis=1)


def whiten(packed, damp, total):
    count = packed.shape[0]
    return pl.pallas_call(
        functools.partial(whiten_kernel, total, count),
        in_specs=[pl.BlockSpec(memory_space=pltpu.SMEM), pl.BlockSpec(memory_space=pltpu.VMEM)],
        out_specs=pl.BlockSpec(memory_space=pltpu.VMEM),
        out_shape=jax.ShapeDtypeStruct(packed.shape, jnp.float32),
    )(damp, packed)


def flip(index, step):
    return index + step * (1 - 2 * ((index // step) % 2))


def remote(src, dst, sems, slot, device):
    return pltpu.make_async_remote_copy(
        src_ref=src,
        dst_ref=dst,
        send_sem=sems.at[0, slot],
        recv_sem=sems.at[1, slot],
        device_id=device,
        device_id_type=pl.DeviceIdType.MESH,
    )


def greet(heads, dps):
    barrier = pltpu.get_barrier_semaphore()
    for peer in heads:
        pl.semaphore_signal(barrier, inc=1, device_id={"head": peer}, device_id_type=pl.DeviceIdType.MESH)
    for peer in dps:
        pl.semaphore_signal(barrier, inc=1, device_id={"dp": peer}, device_id_type=pl.DeviceIdType.MESH)
    pl.semaphore_wait(barrier, len(heads) + len(dps))


def part_rows():
    last = HD // 4
    first = (HD - last) // 2
    return (0, first), (first, first), (2 * first, last)


def scatter_kernel(n_head, n_dp, share, rows_ref, weights_ref, out_ref, acc, sent, own_grams, wide, columns, got_a, got_b, got_c, got_z, got_y, sem_in, sem_0, sem_a, sem_b, sem_c, sem_z, sem_y):
    head = lax.axis_index("head")
    dp = lax.axis_index("dp")
    chunks = n_head // 2
    bits = chunks.bit_length() - 1
    mine = head // 2
    core = head % 2
    per_head = share * n_dp
    span = per_head * HD
    peers = [lax.rem(dp + o, n_dp) for o in range(1, n_dp)]
    part_a, part_b, part_c = part_rows()
    up = list(range(bits))
    down = up[::-1]
    rows_c = pl.ds(part_c[0], part_c[1])

    def chunk_of(e):
        chunk = mine
        for j in range(bits):
            if (e >> j) & 1:
                chunk = chunk + (1 - 2 * ((mine // (1 << j)) % 2)) * (1 << j)
        return chunk

    order = list(range(chunks))[::-1]
    visits = []
    for e in order:
        visits += [2 * chunk_of(e) + 1 - core, 2 * chunk_of(e) + core]

    def fetch(v):
        start = pl.multiple_of(visits[v] * span, 2 * BLK)
        return pltpu.make_async_copy(rows_ref.at[:, pl.ds(start, span)], columns.at[v % 2], sem_in.at[v % 2])

    fetch(0).start()
    wide[...] = jnp.broadcast_to(weights_ref[...], wide.shape)
    greet([flip(head, 1 << j) for j in range(bits + 1)], peers)

    def multiply(v, out):
        if v + 1 < len(visits):
            fetch(v + 1).start()
        fetch(v).wait()

        def pair(i, carry):
            start = pl.multiple_of(i * 2 * HD, 2 * BLK)
            store_pair(columns[v % 2, :, pl.ds(start, 2 * HD)], wide[...], out, 2 * i)
            return carry

        lax.fori_loop(0, per_head // 2, pair, 0, unroll=2)

    def squeeze(e, j):
        return (e >> (j + 1) << j) | (e & ((1 << j) - 1))

    early = {"a": [], "b": []}
    flight_z = []
    for n, e in enumerate(order):
        c = chunk_of(e)
        multiply(2 * n, sent.at[n])
        copy = remote(sent.at[n], acc.at[c], sem_0, n, {"head": flip(head, 1)})
        copy.start()
        multiply(2 * n + 1, own_grams)
        copy.wait()

        def add(m, carry, c=c):
            acc[c, m] += own_grams[m]
            return carry

        lax.fori_loop(0, per_head, add, 0)
        for name, (start, size), got, sems, j in (("a", part_a, got_a, sem_a, up[0]), ("b", part_b, got_b, sem_b, down[0])):
            if (e >> j) & 1:
                slot = squeeze(e, j)
                out = remote(
                    acc.at[c, pl.ds(0, per_head), pl.ds(start, size)], got.at[slot], sems, slot, {"head": flip(head, 2 << j)}
                )
                out.start()
                early[name].append((out, chunk_of(e ^ (1 << j)), slot))
        for o, peer in enumerate(peers):
            out = remote(
                acc.at[c, pl.ds(peer * share, share), rows_c], got_z.at[o, e], sem_z, o * chunks + e, {"dp": peer}
            )
            out.start()
            flight_z.append(out)

    def begin(part, got, sems, order, step, first, count):
        j = order[step]
        bit = (mine // (1 << j)) % 2
        fixed = 0
        for done in order[:step]:
            fixed = fixed + (mine // (1 << done)) % 2 * (1 << done)
        free = [b for b in range(bits) if b not in order[: step + 1]]
        flight = []
        start, size = part
        offset = sum(chunks >> (s + 1) for s in range(step))
        for e in range(1 << len(free)):
            base = fixed + sum(((e >> i) & 1) << b for i, b in enumerate(free))
            slot = offset + e
            copy = remote(
                acc.at[base + (1 - bit) * (1 << j), pl.ds(first, count), pl.ds(start, size)],
                got.at[slot],
                sems,
                slot,
                {"head": flip(head, 2 << j)},
            )
            copy.start()
            flight.append((copy, base + bit * (1 << j), slot))
        return flight, part, got, first, count

    def finish(state):
        flight, (start, size), got, first, count = state
        for copy, keep, slot in flight:
            copy.wait()

            def add(m, carry, keep=keep, slot=slot):
                acc[keep, first + m, start : start + size] += got[slot, m]
                return carry

            lax.fori_loop(0, count, add, 0)

    own = dp * share
    for step in range(bits):
        if step:
            state_a = begin(part_a, got_a, sem_a, up, step, 0, per_head)
            state_b = begin(part_b, got_b, sem_b, down, step, 0, per_head)
        else:
            state_a = early["a"], part_a, got_a, 0, per_head
            state_b = early["b"], part_b, got_b, 0, per_head
        finish(state_a)
        finish(state_b)
    rows_ab = pl.ds(0, part_c[0])
    flight_y = []
    for o, peer in enumerate(peers):
        copy = remote(acc.at[mine, pl.ds(peer * share, share), rows_ab], got_y.at[o], sem_y, o, {"dp": peer})
        copy.start()
        flight_y.append(copy)
    for copy in flight_z:
        copy.wait()
    for e in range(chunks):

        def add_z(m, carry, c=chunk_of(e), e=e):
            value = acc[c, own + m, part_c[0] :]
            for o in range(len(peers)):
                value += got_z[o, e, m]
            acc[c, own + m, part_c[0] :] = value
            return carry

        lax.fori_loop(0, share, add_z, 0)
    for step in range(bits):
        finish(begin(part_c, got_c, sem_c, up, step, own, share))
    for copy in flight_y:
        copy.wait()

    def add_y(m, carry):
        value = acc[mine, own + m, : part_c[0]]
        for o in range(len(peers)):
            value += got_y[o, m]
        out_ref[m, : part_c[0]] = value
        out_ref[m, part_c[0] :] = acc[mine, own + m, part_c[0] :]
        return carry

    lax.fori_loop(0, share, add_y, 0)


def gram_sums(projected, weights, n_head, n_dp):
    tokens, width = projected.shape
    mats, rows, lanes = width // HD, HD, 2 * BLK
    per_head = mats // n_head
    share = per_head // n_dp
    chunks = n_head // 2
    (_, rows_a), (_, rows_b), (_, rows_c) = part_rows()
    f32 = jnp.float32
    return pl.pallas_call(
        functools.partial(scatter_kernel, n_head, n_dp, share),
        in_specs=[pl.BlockSpec(memory_space=pl.ANY), pl.BlockSpec(memory_space=pltpu.VMEM)],
        out_specs=pl.BlockSpec(memory_space=pltpu.VMEM),
        out_shape=jax.ShapeDtypeStruct((share, rows, lanes), f32),
        scratch_shapes=[
            pltpu.VMEM((chunks, per_head, rows, lanes), f32),
            pltpu.VMEM((chunks, per_head, rows, lanes), f32),
            pltpu.VMEM((per_head, rows, lanes), f32),
            pltpu.VMEM((tokens, 2 * HD), projected.dtype),
            pltpu.VMEM((2, tokens, per_head * HD), projected.dtype),
            pltpu.VMEM((chunks - 1, per_head, rows_a, lanes), f32),
            pltpu.VMEM((chunks - 1, per_head, rows_b, lanes), f32),
            pltpu.VMEM((chunks - 1, share, rows_c, lanes), f32),
            pltpu.VMEM((n_dp - 1, chunks, share, rows_c, lanes), f32),
            pltpu.VMEM((n_dp - 1, share, rows - rows_c, lanes), f32),
            pltpu.SemaphoreType.DMA((2,)),
            pltpu.SemaphoreType.DMA((2, chunks)),
            pltpu.SemaphoreType.DMA((2, chunks - 1)),
            pltpu.SemaphoreType.DMA((2, chunks - 1)),
            pltpu.SemaphoreType.DMA((2, chunks - 1)),
            pltpu.SemaphoreType.DMA((2, (n_dp - 1) * chunks)),
            pltpu.SemaphoreType.DMA((2, n_dp - 1)),
        ],
        compiler_params=pltpu.CompilerParams(collective_id=0, has_side_effects=True, vmem_limit_bytes=60 << 20),
    )(projected, weights)


def gather_kernel(n_dp, share, packed_ref, out_ref, got, sems):
    dp = lax.axis_index("dp")
    peers = [lax.rem(dp + o, n_dp) for o in range(1, n_dp)]
    greet([], peers)
    flight = []
    for o, peer in enumerate(peers):
        copy = remote(packed_ref, got.at[o], sems, o, {"dp": peer})
        copy.start()
        flight.append(copy)
    two = 2 * BLK

    def unpack(source, base):
        def one(m, carry):
            top = source[m, :BLK]
            out_ref[base + m, :BLK, :two] = jnp.where(lax.broadcasted_iota(jnp.int32, (BLK, two), 1) < BLK, top, 0.0)
            out_ref[base + m, BLK:, :two] = source[m, BLK:]
            out_ref[base + m, :two, two:] = jnp.zeros((two, BLK), jnp.float32)
            out_ref[base + m, two:, two:] = top[:, BLK:]
            return carry

        lax.fori_loop(0, share, one, 0)

    unpack(packed_ref, dp * share)
    for o in range(n_dp - 1):
        flight[o].wait()
        unpack(got.at[o], lax.rem(dp + n_dp - 1 - o, n_dp) * share)


def gather(packed, n_dp):
    share, rows, lanes = packed.shape
    return pl.pallas_call(
        functools.partial(gather_kernel, n_dp, share),
        in_specs=[pl.BlockSpec(memory_space=pltpu.VMEM)],
        out_specs=pl.BlockSpec(memory_space=pltpu.VMEM),
        out_shape=jax.ShapeDtypeStruct((n_dp * share, HD, HD), jnp.float32),
        scratch_shapes=[
            pltpu.VMEM((n_dp - 1, share, rows, lanes), jnp.float32),
            pltpu.SemaphoreType.DMA((2, n_dp - 1)),
        ],
        compiler_params=pltpu.CompilerParams(collective_id=1, has_side_effects=True),
    )(packed)


def on_device(projected, weight_exp, damp_exp):
    n_head = lax.axis_size("head")
    n_dp = lax.axis_size("dp")
    mats = projected.shape[1] // HD
    share = mats // (n_head * n_dp)
    total = projected.shape[0] * n_head * n_dp
    weights = jnp.exp2(weight_exp.astype(jnp.float32)).astype(jnp.bfloat16)
    owned = gram_sums(projected, weights[:, None], n_head, n_dp)
    first = (lax.axis_index("head") * n_dp + lax.axis_index("dp")) * share
    damp = jnp.exp2(-lax.dynamic_slice_in_dim(damp_exp, first, share, 0).astype(jnp.float32))
    factors = whiten(owned, damp, float(total))
    return gather(factors, n_dp)


def solution(mesh):
    return jax.shard_map(
        on_device,
        mesh=mesh,
        in_specs=(P(("dp", "head"), None), P(("dp", "head")), P()),
        out_specs=P("head", None, None),
        check_vma=False,
    )
```
